32 devices in a mesh: seq: 16 (over z, y, x), head: 2 (over core).
Axes of the slice: x: 2, y: 2, z: 4, core: 2. Of those that a mesh axis runs over, the one named last changes fastest.
Arguments:
- hidden_state: bfloat16 [8, 4096], replicated, may hold values from -18 to 18
- query_weight: bfloat16 [4096, 2, 2048], P('seq', 'head'), may hold values from -1 to 1
- up_key: bfloat16 [2, 256, 512], P('head'), may hold values from -1 to 1
- up_value: bfloat16 [2, 256, 512], P('head'), may hold values from -0.375 to 0.375
- latent_key: bfloat16 [8, 16384, 2, 256], P(None, 'seq', 'head'), may hold values from -256 to 256
- latent_value: bfloat16 [8, 16384, 2, 256], P(None, 'seq', 'head'), may hold values from -6 to 6
- lengths: int32 [8], replicated, may hold values from 12288 to 16384
- block_mask: int32 [8, 64], P(None, 'seq'), may hold values from 0 to 1, as said below
- out_weight: bfloat16 [2, 2048, 4096], P('head', 'seq'), may hold values from -0.09375 to 0.09375
Outputs:
- attn_out: float32 [8, 4096], replicated
The draws below stay inside these ranges and needn't reach their ends.
Inputs may be any that keep to these rules, and one draw needn't show every extreme that they name: `block_mask`: blocks 0 and 32 of every sequence are valid.
All inputs are finite; a program needn't handle non-finite values.
Results may differ from the reference program's by a relative error of at most 0.0035.
Values sent between devices are 32-bit elements; how exact they have to be, the bound alone decides.
No kernel may reach another device: no remote copies, remote signals or barrier semaphores. Data moves between devices by JAX's collectives and lax.ppermute only.
A program may use at most 64 MiB of HBM per device.

```python
import math
import jax
import jax.numpy as jnp
from jax import lax

D = 4096
HQ = 32
HD = 128
GROUPS = 2
R = 256
BLOCK = 256
B = 8
CTX_TOTAL = 16384
NBLK = 64
KPG = 4
REP = 4
QW = 2048
KW = 512


def common_parts(key):
    state = 3.0 * jax.random.truncated_normal(jax.random.fold_in(key, 11), -6.0, 6.0, (B, D), jnp.float32)
    weight = jax.random.truncated_normal(jax.random.fold_in(key, 12), -6.0, 6.0, (D, GROUPS, QW), jnp.float32) / math.sqrt(D)
    basis = jax.random.truncated_normal(jax.random.fold_in(key, 13), -6.0, 6.0, (GROUPS, R, KW), jnp.float32) / math.sqrt(R)
    return (state.astype(jnp.bfloat16), weight.astype(jnp.bfloat16), basis.astype(jnp.bfloat16))


def draw_hidden_state(key, part):
    return common_parts(key)[0]


def draw_query_weight(key, part):
    return common_parts(key)[1]


def draw_up_key(key, part):
    return common_parts(key)[2]


def draw_latent_key(key, part):
    base = jax.random.truncated_normal(jax.random.fold_in(key, 14), -6.0, 6.0, (B, CTX_TOTAL, GROUPS, R), jnp.float32)
    return base.astype(jnp.bfloat16)


def draw_block_mask(key, part):
    picks = jax.random.randint(jax.random.fold_in(key, 17), (B, NBLK), 0, 4)
    marks = jnp.where(picks > 0, 1, 0).astype(jnp.int32)
    return marks.at[:, 0].set(1).at[:, NBLK // 2].set(1)


def place_ends(array, rng, smallest, high):
    shape = array.shape
    index_at = [jax.random.randint(jax.random.fold_in(rng, axis), (), 0, shape[axis]) for axis in range(len(shape))]
    array = array.at[tuple(index_at)].set(smallest)
    longest = shape.index(max(shape))
    index_at[longest] = (index_at[longest] + 1) % shape[longest]
    return array.at[tuple(index_at)].set(high)


def level_of(stream_key, dims, split, least, top_value):
    loudness, own = 1.0, jax.random.fold_in(stream_key, 6)
    for position, parts in split:
        draws = jnp.exp(jax.random.uniform(jax.random.fold_in(own, position), (parts,), jnp.float32, least / len(split), top_value / len(split)))
        loudness = loudness * jnp.repeat(draws, dims[position] // parts).reshape([-1 if axis == position else 1 for axis in range(len(dims))])
    return loudness


def scatter_about(rng, dims, spread, limit, pieces=(), held_as=jnp.bfloat16):
    drawn = jax.random.normal(rng, dims, jnp.float32) * spread
    if len(pieces) > 0:
        drawn = level_of(rng, dims, pieces, -0.22, 0.18) * drawn
    return jnp.clip(drawn, min=-limit, max=limit).astype(held_as)


def setup_inputs(seed: int = 0) -> dict:
    streams_of = jax.random.split(jax.random.key(seed), 10)
    return {
        "hidden_state": draw_hidden_state(jax.random.fold_in(streams_of[9], 71), 0),
        "query_weight": draw_query_weight(jax.random.fold_in(streams_of[9], 71), 0),
        "up_key": draw_up_key(jax.random.fold_in(streams_of[9], 71), 0),
        "up_value": scatter_about(streams_of[3], (GROUPS, R, KW), R ** -0.5, 0.375, ((0, 2),)),
        "latent_key": draw_latent_key(jax.random.fold_in(streams_of[9], 71), 0),
        "latent_value": scatter_about(streams_of[5], (B, CTX_TOTAL, GROUPS, R), 1.0, 6.0, ((1, 16), (2, 2))),
        "lengths": place_ends(jax.random.randint(streams_of[6], (B,), CTX_TOTAL - CTX_TOTAL // 4, CTX_TOTAL + 1), jax.random.fold_in(streams_of[6], 1), CTX_TOTAL - CTX_TOTAL // 4, CTX_TOTAL).astype(jnp.int32),
        "block_mask": draw_block_mask(jax.random.fold_in(streams_of[9], 71), 0),
        "out_weight": scatter_about(streams_of[8], (GROUPS, QW, D), (HQ * HD) ** -0.5, 0.09375, ((0, 2), (1, 16))),
    }


def reference(hidden_state, query_weight, up_key, up_value, latent_key, latent_value, lengths, block_mask, out_weight):
    highest = lax.Precision.HIGHEST
    query = jnp.dot(hidden_state.astype(jnp.float32), query_weight.reshape(D, GROUPS * QW).astype(jnp.float32), preferred_element_type=jnp.float32)
    query_heads = query.reshape(B, GROUPS, KPG, REP, HD)
    positions = jnp.arange(CTX_TOTAL, dtype=jnp.int32)
    block_full = jnp.repeat(block_mask, BLOCK, axis=1)
    valid = (positions[None, :] < lengths[:, None]) & (block_full > 0)
    key_maps = up_key.astype(jnp.float32).reshape(GROUPS, R, KPG, HD)
    value_maps = up_value.astype(jnp.float32).reshape(GROUPS, R, KPG, HD)
    scale = 1.0 / math.sqrt(HD)

    def one_sequence(items):
        query_one, keys_one, values_one, valid_one = items
        results = []
        for group in range(GROUPS):
            query_latent = jnp.einsum('jrd,ejd->jre', query_one[group], key_maps[group], precision=highest)
            scores = jnp.einsum('jre,ce->jrc', query_latent, keys_one[:, group].astype(jnp.float32), precision=highest) * scale
            mask_one = valid_one[None, None, :]
            top = lax.optimization_barrier(jnp.max(jnp.where(mask_one, scores, -1e+30), axis=-1))
            weights = jnp.where(mask_one, jnp.exp(scores - top[..., None]), 0.0)
            total = lax.optimization_barrier(jnp.sum(weights, axis=-1))
            latent_sum = jnp.einsum('jrc,ce->jre', weights, values_one[:, group].astype(jnp.float32), precision=highest)
            summed = jnp.einsum('jre,ejd->jrd', latent_sum, value_maps[group], precision=highest)
            results.append(summed / total[..., None])
        return jnp.stack(results)
    context = lax.map(one_sequence, (query_heads, latent_key, latent_value, valid))
    context = context.reshape(B, GROUPS * QW).astype(jnp.bfloat16)
    result = jnp.dot(context.astype(jnp.float32), out_weight.reshape(GROUPS * QW, D).astype(jnp.float32), preferred_element_type=jnp.float32)
    return result
```

```python
import math

import jax
import jax.numpy as jnp
from jax import lax
from jax.sharding import PartitionSpec as P

HD = 128
R = 256
BLOCK = 256
KPG = 4
REP = 4
QW = 2048


def swap(part, axis, mask):
    size = lax.axis_size(axis)
    return lax.ppermute(part, axis, [(i, i ^ mask) for i in range(size)])


def offsets(radix):
    return sorted(range(1, radix), reverse=True)


def rounds_of(size):
    radices = []
    while size > 1:
        radix = 4 if size % 4 == 0 else 2
        radices.append(radix)
        size //= radix
    return radices


def exchange_pieces(pieces, axis, stride, radix):
    place = (lax.axis_index(axis) // stride) % radix
    received = [
        swap(lax.dynamic_index_in_dim(pieces, place ^ k, 0, False), axis, k * stride)
        for k in offsets(radix)
    ]
    return [lax.dynamic_index_in_dim(pieces, place, 0, False)] + received


def add_all(parts):
    while len(parts) > 1:
        parts = [a + b for a, b in zip(parts[::2], parts[1::2])] + parts[len(parts) // 2 * 2 :]
    return parts[0]


def gather_pieces(piece, axis, stride, radix):
    place = (lax.axis_index(axis) // stride) % radix
    received = {k: swap(piece, axis, k * stride) for k in offsets(radix)}
    slots = jnp.stack([piece] + [received[k] for k in range(1, radix)])
    bit = 1
    while bit < radix:
        pairs = slots.reshape((radix // (2 * bit), 2, bit) + piece.shape)
        slots = jnp.where((place & bit) > 0, pairs[:, ::-1], pairs).reshape(slots.shape)
        bit *= 2
    return slots


def reduce_all(pieces, axis):
    radices = rounds_of(lax.axis_size(axis))
    part = add_all(exchange_pieces(pieces, axis, 1, radices[0]))
    stride = radices[0]
    for radix in radices[1:]:
        part = add_all([part] + [swap(part, axis, k * stride) for k in offsets(radix)])
        stride *= radix
    return gather_pieces(part, axis, 1, radices[0])


def join_packed(parts):
    peaks = [p[..., 8:, 0:1] for p in parts]
    peak = peaks[0]
    for other in peaks[1:]:
        peak = jnp.maximum(peak, other)
    factors = [jnp.exp(p - peak) for p in peaks]
    total = add_all([p[..., 8:, 1:2] * f for p, f in zip(parts, factors)])
    summed = add_all([p[..., :8, :] * f for p, f in zip(parts, factors)])
    return peak, total, summed


def pack(peak, total, summed):
    stats = jnp.concatenate([peak, total], -1)
    stats = jnp.pad(stats, [(0, 0)] * (stats.ndim - 1) + [(0, summed.shape[-1] - 2)])
    return jnp.concatenate([summed, stats], -2)


def body(
    hidden_state,
    query_weight,
    up_key,
    up_value,
    latent_key,
    latent_value,
    lengths,
    block_mask,
    out_weight,
):
    highest = lax.Precision.HIGHEST
    seq_index = lax.axis_index("seq")
    seq_size = lax.axis_size("seq")
    first = rounds_of(seq_size)[0]
    batch = hidden_state.shape[0]
    dim_rows = query_weight.shape[0]
    state_rows = lax.dynamic_slice_in_dim(hidden_state, seq_index * dim_rows, dim_rows, 1)
    partial_query = jnp.dot(state_rows, query_weight[:, 0, :], preferred_element_type=jnp.float32)
    pieces = partial_query.reshape(batch, first, QW // first).transpose(1, 0, 2)
    query = reduce_all(pieces, "seq").transpose(1, 0, 2).reshape(batch, QW)
    query_heads = query.reshape(batch, KPG, REP, HD)
    keys_lat = latent_key[:, :, 0, :]
    values_lat = latent_value[:, :, 0, :]
    context_len = keys_lat.shape[1]
    positions = seq_index * context_len + jnp.arange(context_len, dtype=jnp.int32)
    block_full = jnp.repeat(block_mask, BLOCK, axis=1)
    valid = (positions[None, :] < lengths[:, None]) & (block_full > 0)
    mask_heads = valid[:, None, None, :]
    scale = 1.0 / math.sqrt(HD)
    key_maps = up_key[0].astype(jnp.float32).reshape(R, KPG, HD)
    query_latent = jnp.einsum("bjrd,ejd->bjre", query_heads, key_maps, precision=highest)
    scores = (
        jnp.einsum("bjre,bce->bjrc", query_latent, keys_lat.astype(jnp.float32), precision=highest)
        * scale
    )
    peak = jnp.max(jnp.where(mask_heads, scores, -1e30), axis=-1)
    weights = jnp.where(mask_heads, jnp.exp(scores - peak[..., None]), 0.0)
    total = jnp.sum(weights, axis=-1)
    value_maps = up_value[0].astype(jnp.float32).reshape(R, KPG, HD)
    latent_sum = jnp.einsum(
        "bjrc,bce->bjre", weights, values_lat.astype(jnp.float32), precision=highest
    )
    summed = jnp.einsum("bjre,ejd->bjrd", latent_sum, value_maps, precision=highest)
    out = finish(peak, total, summed, out_weight[0])
    return out


def finish(peak, total, summed, out_rows):
    seq_size = lax.axis_size("seq")
    batch, features = summed.shape[0], out_rows.shape[1]
    row_count = out_rows.shape[0]
    owners_per_head = HD // row_count
    heads = KPG * REP
    first = rounds_of(seq_size)[0]

    def by_head(a):
        return jnp.moveaxis(a.reshape(batch, heads, -1), 0, 1)

    packed = pack(by_head(peak), by_head(total), by_head(summed))
    packed = jnp.repeat(packed, owners_per_head, axis=0)
    stride, rest = 1, packed
    carry = None
    for radix in rounds_of(seq_size):
        pieces = jnp.moveaxis(rest.reshape((-1, radix) + rest.shape[1:]), 1, 0)
        carry = join_packed(exchange_pieces(pieces, "seq", stride, radix))
        rest = pack(*carry)
        stride *= radix
    peak, total, summed = carry
    context = (summed[0] / total[0]).astype(jnp.bfloat16)
    piece = lax.axis_index("seq") % owners_per_head
    context_rows = lax.dynamic_slice_in_dim(context, piece * row_count, row_count, 1)
    partial = jnp.dot(context_rows, out_rows, preferred_element_type=jnp.float32)
    core_count = lax.axis_size("head")
    halves = partial.reshape(batch, core_count, features // core_count).transpose(1, 0, 2)
    if core_count > 1:
        half = add_all(exchange_pieces(halves, "head", 1, core_count))
    else:
        half = halves[0]
    width = half.shape[1] // first
    pieces = half.reshape(batch, first, width).transpose(1, 0, 2)
    half = reduce_all(pieces, "seq").transpose(1, 0, 2).reshape(half.shape)
    if core_count > 1:
        full = gather_pieces(half, "head", 1, core_count)
    else:
        full = half[None]
    return full.transpose(1, 0, 2).reshape(batch, features)


def solution(mesh):
    in_specs = (
        P(),
        P("seq", "head", None),
        P("head", None, None),
        P("head", None, None),
        P(None, "seq", "head", None),
        P(None, "seq", "head", None),
        P(),
        P(None, "seq"),
        P("head", "seq", None),
    )
    out_specs = P()
    return jax.shard_map(body, mesh=mesh, in_specs=in_specs, out_specs=out_specs, check_vma=False)
```

```python
import math

import jax
import jax.numpy as jnp
from jax import lax
from jax.experimental import pallas as pl
from jax.experimental.pallas import tpu as pltpu
from jax.sharding import PartitionSpec as P

HD = 128
R = 256
BLOCK = 256
KPG = 4
REP = 4
QW = 2048


def add_all(parts):
    while len(parts) > 1:
        parts = [a + b for a, b in zip(parts[::2], parts[1::2])] + parts[len(parts) // 2 * 2 :]
    return parts[0]


def swap_core(part):
    size = lax.axis_size("head")
    return lax.ppermute(part, "head", [(i, i ^ 1) for i in range(size)])


def add_over_seq(part):
    size, cores = lax.axis_size("seq"), lax.axis_size("head")
    steps = [1 << k for k in range(size.bit_length() - 1)]
    other = steps[1::-1] + steps[2:] if len(steps) > 1 else steps
    for even, odd in zip(steps, other):
        pairs = [
            (i * cores + c, (i ^ (odd if c % 2 else even)) * cores + c)
            for i in range(size)
            for c in range(cores)
        ]
        part = part + lax.ppermute(part, ("seq", "head"), pairs)
    return part


def halves_of(x):
    high = x.astype(jnp.bfloat16)
    low = (x - high.astype(jnp.float32)).astype(jnp.bfloat16)
    return jnp.concatenate([high, low], 0)


def folded(x):
    half = x.shape[0] // 2
    return x[:half] + x[half:]


def attend_kernel(info_ref, lengths_ref, blocks_ref, query_ref, key_ref, value_ref, map_ref, out_ref):
    group, context_len, _ = key_ref.shape
    heads = query_ref.shape[1]
    batch = out_ref.shape[1] // 2
    first = pl.program_id(0) * group
    scale = 1.0 / math.sqrt(HD)
    column = lax.broadcasted_iota(jnp.int32, (heads, BLOCK), 1)
    scores, masks = [], []
    for g in range(group):
        raw = lax.dot_general(
            halves_of(query_ref[g]),
            key_ref[g],
            (((1,), (1,)), ((), ())),
            preferred_element_type=jnp.float32,
        )
        scores.append(folded(raw) * scale)
        left = lengths_ref[first + g] - info_ref[0]
        parts = []
        for block in range(context_len // BLOCK):
            limit = jnp.where(blocks_ref[first + g, block] > 0, left - block * BLOCK, 0)
            parts.append(column < limit)
        masks.append(jnp.concatenate(parts, 1))
    lane = lax.broadcasted_iota(jnp.int32, (heads, HD), 1)
    row = lax.broadcasted_iota(jnp.int32, (heads, HD), 0)
    for g in range(group):
        peak = jnp.max(jnp.where(masks[g], scores[g], -1e30), axis=1, keepdims=True)
        weights = jnp.where(masks[g], jnp.exp(scores[g] - peak), 0.0)
        total = jnp.sum(weights, axis=1, keepdims=True)
        latent = folded(
            jnp.dot(halves_of(weights), value_ref[g], preferred_element_type=jnp.float32)
        )
        mapped = folded(jnp.dot(halves_of(latent), map_ref[...], preferred_element_type=jnp.float32))
        summed = jnp.zeros((heads, HD), jnp.float32)
        for j in range(KPG):
            summed = jnp.where(row // REP == j, mapped[:, j * HD : (j + 1) * HD], summed)
        stats = jnp.where(lane == 0, peak, jnp.where(lane == 1, total, 0.0))
        out_ref[:, pl.ds(first + g, 1), :] = summed[:, None, :]
        out_ref[:, pl.ds(batch + first + g, 1), :] = stats[:, None, :]


def attend(start, lengths, blocks, query_latent, keys, values, value_map):
    batch, context_len, rank = keys.shape
    heads = query_latent.shape[1]
    group = 4 if batch % 4 == 0 else 1
    smem = pl.BlockSpec(memory_space=pltpu.SMEM)
    return pl.pallas_call(
        attend_kernel,
        grid=(batch // group,),
        in_specs=[
            smem,
            smem,
            smem,
            pl.BlockSpec((group, heads, rank), lambda i: (i, 0, 0)),
            pl.BlockSpec((group, context_len, rank), lambda i: (i, 0, 0)),
            pl.BlockSpec((group, context_len, rank), lambda i: (i, 0, 0)),
            pl.BlockSpec(value_map.shape, lambda i: (0, 0)),
        ],
        out_specs=pl.BlockSpec((heads, 2 * batch, HD), lambda i: (0, 0, 0)),
        out_shape=jax.ShapeDtypeStruct((heads, 2 * batch, HD), jnp.float32),
        compiler_params=pltpu.CompilerParams(dimension_semantics=("arbitrary",)),
        name="attend",
    )(start, lengths, blocks, query_latent, keys, values, value_map)


def body(
    hidden_state,
    query_weight,
    up_key,
    up_value,
    latent_key,
    latent_value,
    lengths,
    block_mask,
    out_weight,
):
    highest = lax.Precision.HIGHEST
    seq_index = lax.axis_index("seq")
    batch = hidden_state.shape[0]
    dim_rows = query_weight.shape[0]
    state_rows = lax.dynamic_slice_in_dim(hidden_state, seq_index * dim_rows, dim_rows, 1)
    partial_query = jnp.dot(state_rows, query_weight[:, 0, :], preferred_element_type=jnp.float32)
    query = add_over_seq(partial_query)
    query_heads = query.reshape(batch, KPG, REP, HD)
    keys = latent_key[:, :, 0, :]
    values = latent_value[:, :, 0, :]
    key_maps = up_key[0].astype(jnp.float32).reshape(R, KPG, HD)
    query_latent = jnp.einsum("bjrd,ejd->bjre", query_heads, key_maps, precision=highest)
    query_latent = query_latent.reshape(batch, KPG * REP, R)
    start = (seq_index * keys.shape[1]).astype(jnp.int32).reshape(1)
    packed = attend(start, lengths, block_mask, query_latent, keys, values, up_value[0])
    return finish(packed, out_weight[0])


def finish(packed, out_rows):
    row_count, features = out_rows.shape
    batch = packed.shape[1] // 2
    owners = HD // row_count
    parts = lax.all_to_all(jnp.repeat(packed, owners, axis=0), "seq", 0, 0, tiled=True)
    peaks, totals = parts[:, batch:, 0:1], parts[:, batch:, 1:2]
    factors = jnp.exp(peaks - jnp.max(peaks, axis=0, keepdims=True))
    total = jnp.sum(totals * factors, axis=0)
    summed = jnp.sum(parts[:, :batch, :] * factors, axis=0)
    context = (summed / total).astype(jnp.bfloat16)
    if owners > 1:
        piece = lax.axis_index("seq") % owners
        context = lax.dynamic_slice_in_dim(context, piece * row_count, row_count, 1)
    partial = jnp.dot(context, out_rows, preferred_element_type=jnp.float32)
    half = features // 2
    south = lax.axis_index("head") == 0
    low, high = partial[:, :half], partial[:, half:]
    mine = jnp.where(south, low, high) + swap_core(jnp.where(south, high, low))
    mine = add_over_seq(mine)
    theirs = swap_core(mine)
    return jnp.concatenate([jnp.where(south, mine, theirs), jnp.where(south, theirs, mine)], 1)


def solution(mesh):
    in_specs = (
        P(),
        P("seq", "head", None),
        P("head", None, None),
        P("head", None, None),
        P(None, "seq", "head", None),
        P(None, "seq", "head", None),
        P(),
        P(None, "seq"),
        P("head", "seq", None),
    )
    out_specs = P()
    return jax.shard_map(body, mesh=mesh, in_specs=in_specs, out_specs=out_specs, check_vma=False)
```

```python
import math

import jax
import jax.numpy as jnp
from jax import lax
from jax.experimental import pallas as pl
from jax.experimental.pallas import tpu as pltpu
from jax.sharding import PartitionSpec as P

HD = 128
R = 256
BLOCK = 256
KPG = 4
REP = 4
QW = 2048


def add_all(parts):
    while len(parts) > 1:
        parts = [a + b for a, b in zip(parts[::2], parts[1::2])] + parts[len(parts) // 2 * 2 :]
    return parts[0]


def swap_core(part):
    size = lax.axis_size("head")
    return lax.ppermute(part, "head", [(i, i ^ 1) for i in range(size)])


def add_over_seq(part):
    size, cores = lax.axis_size("seq"), lax.axis_size("head")
    steps = [1 << k for k in range(size.bit_length() - 1)]
    other = steps[1::-1] + steps[2:] if len(steps) > 1 else steps
    for even, odd in zip(steps, other):
        pairs = [
            (i * cores + c, (i ^ (odd if c % 2 else even)) * cores + c)
            for i in range(size)
            for c in range(cores)
        ]
        part = part + lax.ppermute(part, ("seq", "head"), pairs)
    return part


def halves_of(x):
    high = x.astype(jnp.bfloat16)
    low = (x - high.astype(jnp.float32)).astype(jnp.bfloat16)
    return jnp.concatenate([high, low], 0)


def folded(x):
    half = x.shape[0] // 2
    return x[:half] + x[half:]


def attend_kernel(info_ref, lengths_ref, blocks_ref, query_ref, key_ref, value_ref, map_ref, out_ref):
    group, context_len, _ = key_ref.shape
    heads = query_ref.shape[1]
    batch = out_ref.shape[1] // 2
    first = pl.program_id(0) * group
    scale = 1.0 / math.sqrt(HD)
    column = lax.broadcasted_iota(jnp.int32, (heads, BLOCK), 1)
    scores, masks = [], []
    for g in range(group):
        raw = lax.dot_general(
            halves_of(query_ref[g]),
            key_ref[g],
            (((1,), (1,)), ((), ())),
            preferred_element_type=jnp.float32,
        )
        scores.append(folded(raw) * scale)
        left = lengths_ref[first + g] - info_ref[0]
        parts = []
        for block in range(context_len // BLOCK):
            limit = jnp.where(blocks_ref[first + g, block] > 0, left - block * BLOCK, 0)
            parts.append(column < limit)
        masks.append(jnp.concatenate(parts, 1))
    lane = lax.broadcasted_iota(jnp.int32, (heads, HD), 1)
    row = lax.broadcasted_iota(jnp.int32, (heads, HD), 0)
    for g in range(group):
        peak = jnp.max(jnp.where(masks[g], scores[g], -1e30), axis=1, keepdims=True)
        weights = jnp.where(masks[g], jnp.exp(scores[g] - peak), 0.0)
        total = jnp.sum(weights, axis=1, keepdims=True)
        latent = folded(
            jnp.dot(halves_of(weights), value_ref[g], preferred_element_type=jnp.float32)
        )
        mapped = folded(jnp.dot(halves_of(latent), map_ref[...], preferred_element_type=jnp.float32))
        summed = jnp.zeros((heads, HD), jnp.float32)
        for j in range(KPG):
            summed = jnp.where(row // REP == j, mapped[:, j * HD : (j + 1) * HD], summed)
        stats = jnp.where(lane == 0, peak, jnp.where(lane == 1, total, 0.0))
        out_ref[:, pl.ds(first + g, 1), :] = summed[:, None, :]
        out_ref[:, pl.ds(batch + first + g, 1), :] = stats[:, None, :]


def attend(start, lengths, blocks, query_latent, keys, values, value_map):
    batch, context_len, rank = keys.shape
    heads = query_latent.shape[1]
    group = 2 if batch % 2 == 0 else 1
    smem = pl.BlockSpec(memory_space=pltpu.SMEM)
    return pl.pallas_call(
        attend_kernel,
        grid=(batch // group,),
        in_specs=[
            smem,
            smem,
            smem,
            pl.BlockSpec((group, heads, rank), lambda i: (i, 0, 0)),
            pl.BlockSpec((group, context_len, rank), lambda i: (i, 0, 0)),
            pl.BlockSpec((group, context_len, rank), lambda i: (i, 0, 0)),
            pl.BlockSpec(value_map.shape, lambda i: (0, 0)),
        ],
        out_specs=pl.BlockSpec((heads, 2 * batch, HD), lambda i: (0, 0, 0)),
        out_shape=jax.ShapeDtypeStruct((heads, 2 * batch, HD), jnp.float32),
        compiler_params=pltpu.CompilerParams(dimension_semantics=("arbitrary",)),
        name="attend",
    )(start, lengths, blocks, query_latent, keys, values, value_map)


def body(
    hidden_state,
    query_weight,
    up_key,
    up_value,
    latent_key,
    latent_value,
    lengths,
    block_mask,
    out_weight,
):
    highest = lax.Precision.HIGHEST
    seq_index = lax.axis_index("seq")
    batch = hidden_state.shape[0]
    dim_rows = query_weight.shape[0]
    state_rows = lax.dynamic_slice_in_dim(hidden_state, seq_index * dim_rows, dim_rows, 1)
    partial_query = jnp.dot(state_rows, query_weight[:, 0, :], preferred_element_type=jnp.float32)
    query = add_over_seq(partial_query)
    query_heads = query.reshape(batch, KPG, REP, HD)
    keys = latent_key[:, :, 0, :]
    values = latent_value[:, :, 0, :]
    key_maps = up_key[0].astype(jnp.float32).reshape(R, KPG, HD)
    query_latent = jnp.einsum("bjrd,ejd->bjre", query_heads, key_maps, precision=highest)
    query_latent = query_latent.reshape(batch, KPG * REP, R)
    start = (seq_index * keys.shape[1]).astype(jnp.int32).reshape(1)
    packed = attend(start, lengths, block_mask, query_latent, keys, values, up_value[0])
    return finish(packed, out_weight[0])


def finish(packed, out_rows):
    row_count, features = out_rows.shape
    batch = packed.shape[1] // 2
    owners = HD // row_count
    parts = lax.all_to_all(jnp.repeat(packed, owners, axis=0), "seq", 0, 0, tiled=True)
    peaks, totals = parts[:, batch:, 0:1], parts[:, batch:, 1:2]
    factors = jnp.exp(peaks - jnp.max(peaks, axis=0, keepdims=True))
    total = jnp.sum(totals * factors, axis=0)
    summed = jnp.sum(parts[:, :batch, :] * factors, axis=0)
    context = (summed / total).astype(jnp.bfloat16)
    if owners > 1:
        piece = lax.axis_index("seq") % owners
        context = lax.dynamic_slice_in_dim(context, piece * row_count, row_count, 1)
    partial = jnp.dot(context, out_rows, preferred_element_type=jnp.float32)
    half = features // 2
    south = lax.axis_index("head") == 0
    low, high = partial[:, :half], partial[:, half:]
    mine = jnp.where(south, low, high) + swap_core(jnp.where(south, high, low))
    mine = add_over_seq(mine)
    theirs = swap_core(mine)
    return jnp.concatenate([jnp.where(south, mine, theirs), jnp.where(south, theirs, mine)], 1)


def solution(mesh):
    in_specs = (
        P(),
        P("seq", "head", None),
        P("head", None, None),
        P("head", None, None),
        P(None, "seq", "head", None),
        P(None, "seq", "head", None),
        P(),
        P(None, "seq"),
        P("head", "seq", None),
    )
    out_specs = P()
    return jax.shard_map(body, mesh=mesh, in_specs=in_specs, out_specs=out_specs, check_vma=False)
```
